256 devices in a mesh: grp: 4 (over y, x), seq: 32 (over z), head: 2 (over core).
Axes of the slice: x: 2, y: 2, z: 32, core: 2. Of those that a mesh axis runs over, the one named last changes fastest.
The devices are a block of a 4x8x32 slice.
Arguments:
- inputs: float32 [32768, 4096], P(('grp', 'seq'), 'head'), parts along dimension 0, may hold values from -6 to 6
- rates: float32 [64, 32768], P('head', ('grp', 'seq')), parts along dimension 1, may hold values from 0.5 to 2
- decay_rate: float32 [64], P('head'), may hold values from 0.00012207031 to 0.03
- skip: float32 [64], P('head'), may hold values from 0.5 to 1.5
- keys_b: float32 [32768, 128], P(('grp', 'seq')), parts along dimension 0, may hold values from -0.5 to 0.5
- keys_c: float32 [32768, 128], P(('grp', 'seq')), parts along dimension 0, may hold values from -0.5 to 0.5
- grad_out: float32 [32768, 4096], P(('grp', 'seq'), 'head'), parts along dimension 0, may hold values from -6 to 6
Outputs:
- output: float32 [32768, 4096], P(('grp', 'seq'), 'head'), parts along dimension 0
- grad_inputs: float32 [32768, 4096], P(('grp', 'seq'), 'head'), parts along dimension 0
- input_key_gradient: float32 [32768, 128], P(('grp', 'seq')), parts along dimension 0
- output_key_gradient: float32 [32768, 128], P(('grp', 'seq')), parts along dimension 0
The draws below stay inside these ranges and needn't reach their ends.
There are 4 independent parts, one for each index of `grp`. The reference program is written for one: setup_inputs(seed, part) draws one part's arguments, and reference() takes and returns one part's arrays. A program takes and returns all parts, laid end to end along the dimension named above; an argument that names none is the same for every part. Nothing has to cross between parts.
All inputs are finite; a program needn't handle non-finite values.
Results may differ from the reference program's by a relative error of at most 0.00016.
Values sent between devices are 32-bit elements; how exact they have to be, the bound alone decides.
No kernel may reach another device: no remote copies, remote signals or barrier semaphores. Data moves between devices by JAX's collectives and lax.ppermute only.
A program may use at most 192 MiB of HBM per device.

```python
import math
import jax
import jax.numpy as jnp
from jax import lax

H = 64
P_SIZE = 64
N = 128
SEQ_LEN = 8192


def steps_of(key, extent, shards, least, high):
    loudness, own = 1.0, jax.random.fold_in(key, 6)
    for position, parts in shards:
        steps = jnp.exp(jax.random.uniform(jax.random.fold_in(own, position), (parts,), jnp.float32, least / len(shards), high / len(shards)))
        loudness = loudness * jnp.repeat(steps, extent[position] // parts).reshape([-1 if axis == position else 1 for axis in range(len(extent))])
    return loudness


def bell_draw(own_key, extent, scale, reach, pieces=(), held_as=jnp.bfloat16):
    drawn = jax.random.normal(own_key, extent, jnp.float32) * scale
    if len(pieces) > 0:
        drawn = steps_of(own_key, extent, pieces, -0.22, 0.18) * drawn
    return jnp.clip(drawn, min=-reach, max=reach).astype(held_as)


def setup_inputs(seed: int = 0, part: int = 0) -> dict:
    streams_of = jax.random.split(jax.random.key(seed), 8)
    part_keys = jax.random.split(jax.random.fold_in(streams_of[7], part), 8)
    inputs = bell_draw(part_keys[0], (SEQ_LEN, H * P_SIZE), 1.0, 6.0, ((0, 32), (1, 2)), jnp.float32)
    rates = jnp.clip(jnp.exp(math.log(2.0) - 1.3862944 * jax.random.uniform(part_keys[1], (H, SEQ_LEN), jnp.float32) ** steps_of(part_keys[1], (H, SEQ_LEN), ((0, 2), (1, 32)), -0.2, 0.2)), 0.5, 2.0)
    decay_rate = jnp.clip(jnp.exp(math.log(0.03) - 5.5043554 * jax.random.uniform(streams_of[2], (H,), jnp.float32) ** steps_of(streams_of[2], (H,), ((0, 2),), -0.2, 0.2)), 0.00012207031, 0.03)
    skip = jnp.clip(0.5 + 1.0 * jax.random.uniform(streams_of[3], (H,), jnp.float32) ** steps_of(streams_of[3], (H,), ((0, 2),), -0.2, 0.2), 0.5, 1.5)
    keys_b = bell_draw(part_keys[4], (SEQ_LEN, N), N ** -0.5, 0.5, ((0, 32),), jnp.float32)
    keys_c = bell_draw(part_keys[5], (SEQ_LEN, N), N ** -0.5, 0.5, ((0, 32),), jnp.float32)
    grad_out = bell_draw(part_keys[6], (SEQ_LEN, H * P_SIZE), 1.0, 6.0, ((0, 32), (1, 2)), jnp.float32)
    return {"inputs": inputs, "rates": rates, "decay_rate": decay_rate, "skip": skip, "keys_b": keys_b, "keys_c": keys_c, "grad_out": grad_out}


HIGH = lax.Precision.HIGHEST


def reference(inputs, rates, decay_rate, skip, keys_b, keys_c, grad_out):
    length = inputs.shape[0]
    heads = rates.shape[0]
    width = inputs.shape[1] // heads
    state_size = keys_b.shape[1]
    input_rows = inputs.reshape(length, heads, width)
    dys = grad_out.reshape(length, heads, width)
    steps = rates.T
    factors = jnp.exp(-steps * decay_rate[None, :])
    items = (input_rows, steps, factors, keys_b, keys_c, dys)

    def ahead(state, item):
        x, step, factor, key_b, key_c, grad = item
        state = factor[:, None, None] * state + (step[:, None] * x)[:, :, None] * key_b[None, None, :]
        out = jnp.einsum("hpn,n->hp", state, key_c, precision=HIGH) + skip[:, None] * x
        output_key_gradient = jnp.einsum("hpn,hp->n", state, grad, precision=HIGH)
        return state, (out, output_key_gradient)

    start = jnp.zeros((heads, width, state_size), jnp.float32)
    unused, (outs, grads_c) = lax.scan(ahead, start, items)

    def behind(carry, item):
        x, step, factor, key_b, key_c, grad = item
        adjoint_state = grad[:, :, None] * key_c[None, None, :] + carry
        grad_x = step[:, None] * jnp.einsum("hpn,n->hp", adjoint_state, key_b, precision=HIGH) + skip[:, None] * grad
        input_key_gradient = jnp.einsum("hpn,hp->n", adjoint_state, step[:, None] * x, precision=HIGH)
        return factor[:, None, None] * adjoint_state, (grad_x, input_key_gradient)

    unused_two, (grads_x, grads_b) = lax.scan(behind, start, items, reverse=True)
    return (outs.reshape(length, heads * width), grads_x.reshape(length, heads * width), grads_b, grads_c)
```

```python
import functools

import jax
import jax.numpy as jnp
from jax import lax
from jax.experimental import pallas as pl
from jax.experimental.pallas import tpu as pltpu
from jax.sharding import PartitionSpec as P

HIGHEST = lax.Precision.HIGHEST
LANES = 256
LEVELS = 3


def halves(a):
    high = a.astype(jnp.bfloat16)
    return high, (a - high.astype(jnp.float32)).astype(jnp.bfloat16)


def dot3(a, b, dims=(((1,), (0,)), ((), ()))):
    dot = functools.partial(lax.dot_general, dimension_numbers=dims, preferred_element_type=jnp.float32)
    return dot(a[0], b[0]) + (dot(a[0], b[1]) + dot(a[1], b[0]))


NT = (((1,), (1,)), ((), ()))
TN = (((0,), (0,)), ((), ()))


def spread(columns, first, width, lanes):
    heads = columns.shape[1]
    row = lax.broadcasted_iota(jnp.int32, (heads, lanes), 0)
    lane = lax.broadcasted_iota(jnp.int32, (heads, lanes), 1)
    chosen = jnp.where(row == first + lane // width, 1.0, 0.0).astype(jnp.float32)
    return jnp.dot(columns, chosen, precision=HIGHEST, preferred_element_type=jnp.float32)


def states_kernel(width, x_ref, dy_ref, tail_ref, growth_ref, b_ref, c_ref, out_ref):
    first = pl.program_id(0) * (LANES // width)
    xs = x_ref[...] * spread(tail_ref[...], first, width, LANES)
    ys = dy_ref[...] * spread(growth_ref[...], first, width, LANES)
    out_ref[0] = dot3(halves(b_ref[...]), halves(xs), TN)
    out_ref[1] = dot3(halves(c_ref[...]), halves(ys), TN)


def local_kernel(width, x_ref, dy_ref, inner_t_ref, rates_t_ref, inner_ref, rates_ref, skip_ref, b_ref, c_ref, y_ref, gx_ref, keys_ref, cb_ref, bc_ref, sum_ref):
    step = pl.program_id(0)
    tokens = x_ref.shape[0]
    per = LANES // width

    @pl.when(step == 0)
    def _():
        b, c = halves(b_ref[...]), halves(c_ref[...])
        cb_ref[...] = dot3(c, b, NT)
        bc_ref[...] = dot3(b, c, NT)
        sum_ref[...] = jnp.zeros_like(sum_ref)

    row = lax.broadcasted_iota(jnp.int32, (tokens, tokens), 0)
    col = lax.broadcasted_iota(jnp.int32, (tokens, tokens), 1)
    lane = lax.broadcasted_iota(jnp.int32, (tokens, 2 * width), 1)
    total = sum_ref[...]
    for pair in range(per // 2):
        at = slice(pair * 2 * width, (pair + 1) * 2 * width)
        x, dy = x_ref[:, at], dy_ref[:, at]
        y = skip_ref[:, at] * x
        gx = skip_ref[:, at] * dy
        x_parts, dy_parts = halves(x), halves(dy)
        for side in range(2):
            i = pair * 2 + side
            mine = (lane < width) if side == 0 else (lane >= width)
            zero = jnp.zeros((), jnp.bfloat16)
            x_own = tuple(jnp.where(mine, part, zero) for part in x_parts)
            dy_own = tuple(jnp.where(mine, part, zero) for part in dy_parts)
            down = spread(inner_t_ref[...], step * per + i, tokens, tokens)
            dt_down = spread(rates_t_ref[...], step * per + i, tokens, tokens)
            across = inner_ref[0, i : i + 1, :]
            gap = down - across
            within = jnp.where(row >= col, jnp.exp(jnp.minimum(gap, 0.0)), 0.0) * rates_ref[0, i : i + 1, :]
            turned = jnp.where(col >= row, jnp.exp(jnp.minimum(-gap, 0.0)), 0.0) * dt_down
            y = y + dot3(halves(within * cb_ref[...]), x_own)
            gx = gx + dot3(halves(turned * bc_ref[...]), dy_own)
            total = total + within * dot3(dy_own, x_parts, NT)
        y_ref[:, at] = y
        gx_ref[:, at] = gx
    sum_ref[...] = total

    @pl.when(step == pl.num_programs(0) - 1)
    def _():
        parts = halves(sum_ref[...])
        keys_ref[:tokens] = dot3(parts, halves(c_ref[...]), TN)
        keys_ref[tokens:] = dot3(parts, halves(b_ref[...]))


def finish_kernel(width, x_ref, dy_ref, tail_ref, growth_ref, b_ref, c_ref, low_ref, high_ref, y_ref, gx_ref, terms_ref, out_ref, grad_ref, keys_ref):
    step = pl.program_id(0)
    tokens = x_ref.shape[0]
    first = step * (LANES // width)
    tail = spread(tail_ref[...], first, width, LANES)
    growth = spread(growth_ref[...], first, width, LANES)
    entering, adjoint = (halves(jnp.concatenate([low_ref[i], high_ref[i]], axis=0)) for i in range(2))
    out_ref[...] = y_ref[...] + growth * dot3(halves(c_ref[...]), entering)
    grad_ref[...] = gx_ref[...] + tail * dot3(halves(b_ref[...]), adjoint)

    @pl.when(step == 0)
    def _():
        keys_ref[...] = terms_ref[...]

    keys_ref[:tokens] += dot3(halves(x_ref[...] * tail), adjoint, NT)
    keys_ref[tokens:] += dot3(halves(dy_ref[...] * growth), entering, NT)


def whole(shape):
    return pl.BlockSpec(shape, lambda i: (0,) * len(shape))


def span(weights, table):
    return jnp.exp(jnp.dot(weights, table, precision=HIGHEST))


def exchange(states, log_decay, spread_lanes, axis, meanwhile):
    size, mine = lax.axis_size(axis), lax.axis_index(axis)
    heads = log_decay.shape[0]
    table = jnp.zeros((size, 128), jnp.float32)
    table = lax.dynamic_update_slice(table, jnp.pad(log_decay, (0, 128 - heads))[None], (mine, 0))
    seg = jnp.arange(size)
    steps = size.bit_length() - 1
    tables = []
    for k in range(steps):
        table = table + lax.ppermute(table, axis, [(i, i ^ (1 << k)) for i in range(size)])
        tables.append(table)

    def weights(masks, known):
        rows = span(jnp.stack(masks).astype(jnp.float32), known)
        return jnp.dot(rows, spread_lanes, precision=HIGHEST)

    kept, sides = [], []
    now = states
    for k in range(LEVELS):
        pairs = [(i, i ^ (1 << k)) for i in range(size)]
        right = ((mine >> k) & 1) == 1
        base = (mine >> (k + 1)) << (k + 1)
        half = 1 << k
        both = weights(
            [(seg >= base) & (seg < base + half), (seg >= base + half) & (seg < base + 2 * half)], tables[k]
        )
        over_left, over_right = both[0:1], both[1:2]
        rows = now.shape[1] // 2
        low, high = now[:, :rows], now[:, rows:]
        own = jnp.where(right, high, low)
        got = lax.ppermute(jnp.where(right, low, high), axis, pairs)
        left_part, right_part = jnp.where(right, got, own), jnp.where(right, own, got)
        now = jnp.stack(
            [over_right * left_part[0] + right_part[0], left_part[1] + over_left * right_part[1]]
        )
        kept.append((left_part[0], right_part[1], over_left, over_right))
        sides.append((pairs, right))

    block = 1 << LEVELS
    count = size // block
    place = mine // block
    forward = jnp.zeros_like(now[0])
    backward = jnp.zeros_like(now[0])
    masks, received = [], []
    for d in range(1, count):
        pairs = [(i, (i + block * d) % size) for i in range(size)]
        received.append(lax.ppermute(jnp.where(place + d < count, now[0], now[1]), axis, pairs))
        source = (place - d) % count
        first, last = jnp.minimum(source, place), jnp.maximum(source, place)
        masks.append((seg // block > first) & (seg // block < last))
    between = weights(masks, tables[-1])
    aside = meanwhile(now)
    received, aside = lax.optimization_barrier((received, aside))
    for d in range(1, count):
        term = between[d - 1 : d] * received[d - 1]
        forward = forward + jnp.where(place >= d, term, 0.0)
        backward = backward + jnp.where(place >= d, 0.0, term)

    for k in reversed(range(LEVELS)):
        left_sum, right_sum, over_left, over_right = kept[k]
        pairs, right = sides[k]
        to_left = jnp.stack([forward, over_right * backward + right_sum])
        to_right = jnp.stack([over_left * forward + left_sum, backward])
        own = jnp.where(right, to_right, to_left)
        got = lax.ppermute(jnp.where(right, to_left, to_right), axis, pairs)
        low, high = jnp.where(right, got, own), jnp.where(right, own, got)
        if k:
            forward, backward = (jnp.concatenate([low[i], high[i]], axis=0) for i in range(2))
    return (low, high), aside


def body(inputs, rates, decay_rate, skip, keys_b, keys_c, grad_out):
    tokens, lanes = inputs.shape
    heads = rates.shape[0]
    width = lanes // heads
    state_size = keys_b.shape[1]
    grid = lanes // LANES
    per = LANES // width

    logs = -(decay_rate[:, None] * rates)
    upto = jnp.triu(jnp.ones((tokens, tokens), jnp.float32))
    inner = jnp.dot(logs, upto, precision=HIGHEST)
    total = jnp.sum(logs, axis=1)
    inner_t = inner.T
    rates_t = rates.T
    growth_t = jnp.exp(inner_t)
    tail_t = jnp.exp(jnp.minimum(total[None, :] - inner_t, 0.0)) * rates_t
    head_of = jnp.arange(lanes) // width
    spread_lanes = (jnp.arange(128)[:, None] == head_of[None, :]).astype(jnp.float32)
    skip_lanes = jnp.dot(jnp.pad(skip, (0, 128 - heads))[None], spread_lanes, precision=HIGHEST)

    tile = pl.BlockSpec((tokens, LANES), lambda i: (0, i))
    state_tile = pl.BlockSpec((2, state_size, LANES), lambda i: (0, 0, i))
    half_tile = pl.BlockSpec((2, state_size // 2, LANES), lambda i: (0, 0, i))
    columns = whole((tokens, heads))
    keys = whole((tokens, state_size))
    big = jax.ShapeDtypeStruct((tokens, lanes), jnp.float32)
    params = pltpu.CompilerParams(dimension_semantics=("arbitrary",))

    states = pl.pallas_call(
        functools.partial(states_kernel, width),
        grid=(grid,),
        in_specs=[tile, tile, columns, columns, keys, keys],
        out_specs=state_tile,
        out_shape=jax.ShapeDtypeStruct((2, state_size, lanes), jnp.float32),
        compiler_params=params,
        cost_estimate=pl.CostEstimate(flops=12 * tokens * state_size * lanes, bytes_accessed=6 << 20, transcendentals=0),
        name="states",
    )(inputs, grad_out, tail_t, growth_t, keys_b, keys_c)

    small = pl.BlockSpec((1, per, tokens), lambda i: (i, 0, 0))
    local = pl.pallas_call(
        functools.partial(local_kernel, width),
        grid=(grid,),
        in_specs=[tile, tile, columns, columns, small, small, pl.BlockSpec((1, LANES), lambda i: (0, i)), keys, keys],
        out_specs=[tile, tile, whole((2 * tokens, state_size))],
        out_shape=[big, big, jax.ShapeDtypeStruct((2 * tokens, state_size), jnp.float32)],
        scratch_shapes=[pltpu.VMEM((tokens, tokens), jnp.float32)] * 3,
        compiler_params=params,
        cost_estimate=pl.CostEstimate(flops=18 * tokens * tokens * lanes, bytes_accessed=8 << 20, transcendentals=2 * tokens * tokens * heads),
        name="local",
    )
    by_step = inner.reshape(grid, per, tokens), rates.reshape(grid, per, tokens)

    def meanwhile(after):
        x, _ = lax.optimization_barrier((inputs, after))
        return local(x, grad_out, inner_t, rates_t, *by_step, skip_lanes, keys_b, keys_c)

    (low, high), (y, gx, terms) = exchange(states, total, spread_lanes, "seq", meanwhile)

    output, grad_x, key_terms = pl.pallas_call(
        functools.partial(finish_kernel, width),
        grid=(grid,),
        in_specs=[tile, tile, columns, columns, keys, keys, half_tile, half_tile, tile, tile, whole((2 * tokens, state_size))],
        out_specs=[tile, tile, whole((2 * tokens, state_size))],
        out_shape=[big, big, jax.ShapeDtypeStruct((2 * tokens, state_size), jnp.float32)],
        compiler_params=pltpu.CompilerParams(dimension_semantics=("arbitrary",), vmem_limit_bytes=20 << 20),
        cost_estimate=pl.CostEstimate(flops=24 * tokens * state_size * lanes, bytes_accessed=14 << 20, transcendentals=0),
        name="finish",
    )(inputs, grad_out, tail_t, growth_t, keys_b, keys_c, low, high, y, gx, terms)
    cores = lax.axis_size("head")
    summed = key_terms
    for d in range(1, cores):
        summed = summed + lax.ppermute(key_terms, "head", [(i, (i + d) % cores) for i in range(cores)])
    return output, grad_x, summed[:tokens], summed[tokens:]


def solution(mesh):
    in_specs = (
        P(("grp", "seq"), "head"),
        P("head", ("grp", "seq")),
        P("head"),
        P("head"),
        P(("grp", "seq"), None),
        P(("grp", "seq"), None),
        P(("grp", "seq"), "head"),
    )
    out_specs = (
        P(("grp", "seq"), "head"),
        P(("grp", "seq"), "head"),
        P(("grp", "seq"), None),
        P(("grp", "seq"), None),
    )
    return jax.shard_map(body, mesh=mesh, in_specs=in_specs, out_specs=out_specs, check_vma=False)
```

```python
import functools

import jax
import jax.numpy as jnp
from jax import lax
from jax.experimental import pallas as pl
from jax.experimental.pallas import tpu as pltpu
from jax.sharding import PartitionSpec as P

HIGHEST = lax.Precision.HIGHEST
LANES = 256
LEVELS = 3


def halves(a):
    high = a.astype(jnp.bfloat16)
    return high, (a - high.astype(jnp.float32)).astype(jnp.bfloat16)


def dot3(a, b, dims=(((1,), (0,)), ((), ()))):
    dot = functools.partial(lax.dot_general, dimension_numbers=dims, preferred_element_type=jnp.float32)
    return dot(a[0], b[0]) + (dot(a[0], b[1]) + dot(a[1], b[0]))


NT = (((1,), (1,)), ((), ()))
TN = (((0,), (0,)), ((), ()))


def spread(columns, width):
    tokens, heads = columns.shape
    lane = lax.broadcasted_iota(jnp.int32, (tokens, 2 * width), 1)
    pairs = [jnp.where(lane < width, columns[:, i : i + 1], columns[:, i + 1 : i + 2]) for i in range(0, heads, 2)]
    return jnp.concatenate(pairs, axis=1)


def scales(inner_ref, rates_ref, width):
    inner = inner_ref[0]
    tail = jnp.exp(jnp.minimum(inner[-1:] - inner, 0.0)) * rates_ref[0]
    return spread(tail, width), spread(jnp.exp(inner), width)


def states_kernel(width, x_ref, dy_ref, inner_ref, rates_ref, b_ref, c_ref, out_ref):
    tail, growth = scales(inner_ref, rates_ref, width)
    for i, (keys_ref, rows) in enumerate(((b_ref, x_ref[...] * tail), (c_ref, dy_ref[...] * growth))):
        state = dot3(halves(keys_ref[...]), halves(rows), TN)
        for j in range(LANES // 128):
            out_ref[i, :, j] = state[:, j * 128 : (j + 1) * 128].reshape(-1, 8, 128)


def local_kernel(width, x_ref, dy_ref, inner_t_ref, rates_t_ref, inner_ref, rates_ref, skip_ref, b_ref, c_ref, y_ref, gx_ref, keys_ref, cb_ref, bc_ref, sum_ref):
    step = pl.program_id(0)
    tokens = x_ref.shape[0]
    per = LANES // width

    @pl.when(step == 0)
    def _():
        b, c = halves(b_ref[...]), halves(c_ref[...])
        cb_ref[...] = dot3(c, b, NT)
        bc_ref[...] = dot3(b, c, NT)
        sum_ref[...] = jnp.zeros_like(sum_ref)

    row = lax.broadcasted_iota(jnp.int32, (tokens, tokens), 0)
    col = lax.broadcasted_iota(jnp.int32, (tokens, tokens), 1)
    lane = lax.broadcasted_iota(jnp.int32, (tokens, 2 * width), 1)
    total = sum_ref[...]
    for pair in range(per // 2):
        at = slice(pair * 2 * width, (pair + 1) * 2 * width)
        x, dy = x_ref[:, at], dy_ref[:, at]
        y = skip_ref[:, at] * x
        gx = skip_ref[:, at] * dy
        x_parts, dy_parts = halves(x), halves(dy)
        for side in range(2):
            i = pair * 2 + side
            mine = (lane < width) if side == 0 else (lane >= width)
            zero = jnp.zeros((), jnp.bfloat16)
            x_own = tuple(jnp.where(mine, part, zero) for part in x_parts)
            dy_own = tuple(jnp.where(mine, part, zero) for part in dy_parts)
            down = jnp.broadcast_to(inner_t_ref[0, :, i : i + 1], (tokens, tokens))
            dt_down = jnp.broadcast_to(rates_t_ref[0, :, i : i + 1], (tokens, tokens))
            across = inner_ref[0, i : i + 1, :]
            gap = down - across
            within = jnp.where(row >= col, jnp.exp(jnp.minimum(gap, 0.0)), 0.0) * rates_ref[0, i : i + 1, :]
            turned = jnp.where(col >= row, jnp.exp(jnp.minimum(-gap, 0.0)), 0.0) * dt_down
            y = y + dot3(halves(within * cb_ref[...]), x_own)
            gx = gx + dot3(halves(turned * bc_ref[...]), dy_own)
            total = total + within * dot3(dy_own, x_parts, NT)
        y_ref[:, at] = y
        gx_ref[:, at] = gx
    sum_ref[...] = total

    @pl.when(step == pl.num_programs(0) - 1)
    def _():
        parts = halves(sum_ref[...])
        keys_ref[:tokens] = dot3(parts, halves(c_ref[...]), TN)
        keys_ref[tokens:] = dot3(parts, halves(b_ref[...]))


def finish_kernel(width, x_ref, dy_ref, inner_ref, rates_ref, b_ref, c_ref, low_ref, high_ref, y_ref, gx_ref, terms_ref, out_ref, grad_ref, keys_ref):
    step = pl.program_id(0)
    tokens = x_ref.shape[0]
    tail, growth = scales(inner_ref, rates_ref, width)

    def state(i):
        rows = [
            jnp.concatenate([ref[i, :, j].reshape(-1, 128) for j in range(LANES // 128)], axis=1)
            for ref in (low_ref, high_ref)
        ]
        return halves(jnp.concatenate(rows, axis=0))

    entering, adjoint = state(0), state(1)
    out_ref[...] = y_ref[...] + growth * dot3(halves(c_ref[...]), entering)
    grad_ref[...] = gx_ref[...] + tail * dot3(halves(b_ref[...]), adjoint)

    @pl.when(step == 0)
    def _():
        keys_ref[...] = terms_ref[...]

    keys_ref[:tokens] += dot3(halves(x_ref[...] * tail), adjoint, NT)
    keys_ref[tokens:] += dot3(halves(dy_ref[...] * growth), entering, NT)


def whole(shape):
    return pl.BlockSpec(shape, lambda i: (0,) * len(shape))


def exchange(states, log_decay, axis, meanwhile):
    size, mine = lax.axis_size(axis), lax.axis_index(axis)
    tiles = log_decay.shape[0]

    def send(values, logs, pairs):
        got = lax.ppermute(jnp.concatenate([values.reshape(-1, 128), logs], axis=0), axis, pairs)
        return got[:-tiles].reshape(values.shape), got[-tiles:]

    def decay(logs):
        return jnp.exp(logs)[None, :, None, :]

    kept, sides = [], []
    now, logs = states, log_decay
    for k in range(LEVELS):
        pairs = [(i, i ^ (1 << k)) for i in range(size)]
        right = ((mine >> k) & 1) == 1
        rows = now.shape[1] // 2
        low, high = now[:, :rows], now[:, rows:]
        own = jnp.where(right, high, low)
        got, other = send(jnp.where(right, low, high), logs, pairs)
        left_logs, right_logs = jnp.where(right, other, logs), jnp.where(right, logs, other)
        over_left, over_right = decay(left_logs), decay(right_logs)
        left_part, right_part = jnp.where(right, got, own), jnp.where(right, own, got)
        now = jnp.stack(
            [over_right * left_part[0] + right_part[0], left_part[1] + over_left * right_part[1]]
        )
        logs = left_logs + right_logs
        kept.append((left_part[0], right_part[1], over_left, over_right))
        sides.append((pairs, right))

    block = 1 << LEVELS
    count = size // block
    place = mine // block
    received, sources = [], []
    for d in range(1, count):
        pairs = [(i, (i + block * d) % size) for i in range(size)]
        received.append(send(jnp.where(place + d < count, now[0], now[1]), logs, pairs))
        sources.append((place - d) % count)
    aside = meanwhile()
    forward = jnp.zeros_like(now[0])
    backward = jnp.zeros_like(now[0])
    for d in range(1, count):
        first, last = jnp.minimum(sources[d - 1], place), jnp.maximum(sources[d - 1], place)
        between = jnp.zeros_like(logs)
        for (_, other), source in zip(received, sources, strict=True):
            between = between + jnp.where((source > first) & (source < last), other, 0.0)
        term = decay(between) * received[d - 1][0]
        forward = forward + jnp.where(place >= d, term, 0.0)
        backward = backward + jnp.where(place >= d, 0.0, term)

    for k in reversed(range(LEVELS)):
        left_sum, right_sum, over_left, over_right = kept[k]
        pairs, right = sides[k]
        to_left = jnp.stack([forward, over_right * backward + right_sum])
        to_right = jnp.stack([over_left * forward + left_sum, backward])
        own = jnp.where(right, to_right, to_left)
        got = lax.ppermute(jnp.where(right, to_left, to_right), axis, pairs)
        low, high = jnp.where(right, got, own), jnp.where(right, own, got)
        if k:
            forward, backward = (jnp.concatenate([low[i], high[i]], axis=0) for i in range(2))
    return (low, high), aside


def body(inputs, rates, decay_rate, skip, keys_b, keys_c, grad_out):
    tokens, lanes = inputs.shape
    heads = rates.shape[0]
    width = lanes // heads
    state_size = keys_b.shape[1]
    grid = lanes // LANES
    per = LANES // width

    logs = -(decay_rate[:, None] * rates)
    upto = jnp.triu(jnp.ones((tokens, tokens), jnp.float32))
    inner = jnp.dot(logs, upto, precision=HIGHEST)
    total = jnp.sum(logs, axis=1)
    inner_rows, rates_rows = inner.reshape(grid, per, tokens), rates.reshape(grid, per, tokens)
    inner_t, rates_t = jnp.swapaxes(inner_rows, 1, 2), jnp.swapaxes(rates_rows, 1, 2)

    def on_lanes(of_heads):
        lane = jnp.arange(lanes).reshape(lanes // 128, 128, 1)
        return jnp.sum(jnp.where(lane // width == jnp.arange(heads), of_heads, 0.0), axis=2)

    tile = pl.BlockSpec((tokens, LANES), lambda i: (0, i))
    state_tile = pl.BlockSpec((2, state_size // 8, LANES // 128, 8, 128), lambda i: (0, 0, i, 0, 0))
    half_tile = pl.BlockSpec((2, state_size // 16, LANES // 128, 8, 128), lambda i: (0, 0, i, 0, 0))
    columns = pl.BlockSpec((1, tokens, per), lambda i: (i, 0, 0))
    keys = whole((tokens, state_size))
    big = jax.ShapeDtypeStruct((tokens, lanes), jnp.float32)
    params = pltpu.CompilerParams(dimension_semantics=("arbitrary",))

    states = pl.pallas_call(
        functools.partial(states_kernel, width),
        grid=(grid,),
        in_specs=[tile, tile, columns, columns, keys, keys],
        out_specs=state_tile,
        out_shape=jax.ShapeDtypeStruct((2, state_size // 8, lanes // 128, 8, 128), jnp.float32),
        compiler_params=params,
        cost_estimate=pl.CostEstimate(flops=12 * tokens * state_size * lanes, bytes_accessed=6 << 20, transcendentals=0),
        name="states",
    )(inputs, grad_out, inner_t, rates_t, keys_b, keys_c)

    small = pl.BlockSpec((1, per, tokens), lambda i: (i, 0, 0))
    local = pl.pallas_call(
        functools.partial(local_kernel, width),
        grid=(grid,),
        in_specs=[tile, tile, columns, columns, small, small, pl.BlockSpec((1, LANES), lambda i: (0, i)), keys, keys],
        out_specs=[tile, tile, whole((2 * tokens, state_size))],
        out_shape=[big, big, jax.ShapeDtypeStruct((2 * tokens, state_size), jnp.float32)],
        scratch_shapes=[pltpu.VMEM((tokens, tokens), jnp.float32)] * 3,
        compiler_params=params,
        cost_estimate=pl.CostEstimate(flops=18 * tokens * tokens * lanes, bytes_accessed=8 << 20, transcendentals=2 * tokens * tokens * heads),
        name="local",
    )
    skip_lanes = on_lanes(skip).reshape(1, lanes)

    def meanwhile():
        return local(inputs, grad_out, inner_t, rates_t, inner_rows, rates_rows, skip_lanes, keys_b, keys_c)

    (low, high), (y, gx, terms) = exchange(states, on_lanes(total), "seq", meanwhile)

    output, grad_x, key_terms = pl.pallas_call(
        functools.partial(finish_kernel, width),
        grid=(grid,),
        in_specs=[tile, tile, columns, columns, keys, keys, half_tile, half_tile, tile, tile, whole((2 * tokens, state_size))],
        out_specs=[tile, tile, whole((2 * tokens, state_size))],
        out_shape=[big, big, jax.ShapeDtypeStruct((2 * tokens, state_size), jnp.float32)],
        compiler_params=pltpu.CompilerParams(dimension_semantics=("arbitrary",), vmem_limit_bytes=20 << 20),
        cost_estimate=pl.CostEstimate(flops=24 * tokens * state_size * lanes, bytes_accessed=14 << 20, transcendentals=0),
        name="finish",
    )(inputs, grad_out, inner_t, rates_t, keys_b, keys_c, low, high, y, gx, terms)
    cores = lax.axis_size("head")
    summed = key_terms
    for d in range(1, cores):
        summed = summed + lax.ppermute(key_terms, "head", [(i, (i + d) % cores) for i in range(cores)])
    return output, grad_x, summed[:tokens], summed[tokens:]


def solution(mesh):
    in_specs = (
        P(("grp", "seq"), "head"),
        P("head", ("grp", "seq")),
        P("head"),
        P("head"),
        P(("grp", "seq"), None),
        P(("grp", "seq"), None),
        P(("grp", "seq"), "head"),
    )
    out_specs = (
        P(("grp", "seq"), "head"),
        P(("grp", "seq"), "head"),
        P(("grp", "seq"), None),
        P(("grp", "seq"), None),
    )
    return jax.shard_map(body, mesh=mesh, in_specs=in_specs, out_specs=out_specs, check_vma=False)
```

```python
import functools

import jax
import jax.numpy as jnp
from jax import lax
from jax.experimental import pallas as pl
from jax.experimental.pallas import tpu as pltpu
from jax.sharding import PartitionSpec as P

HIGHEST = lax.Precision.HIGHEST
LANES = 256
LEVELS = 3


def halves(a):
    high = a.astype(jnp.bfloat16)
    return high, (a - high.astype(jnp.float32)).astype(jnp.bfloat16)


def dot3(a, b, dims=(((1,), (0,)), ((), ()))):
    dot = functools.partial(lax.dot_general, dimension_numbers=dims, preferred_element_type=jnp.float32)
    return dot(a[0], b[0]) + (dot(a[0], b[1]) + dot(a[1], b[0]))


NT = (((1,), (1,)), ((), ()))
TN = (((0,), (0,)), ((), ()))


def spread(columns, width):
    tokens, heads = columns.shape
    lane = lax.broadcasted_iota(jnp.int32, (tokens, 2 * width), 1)
    pairs = [jnp.where(lane < width, columns[:, i : i + 1], columns[:, i + 1 : i + 2]) for i in range(0, heads, 2)]
    return jnp.concatenate(pairs, axis=1)


def scales(inner_ref, rates_ref, width):
    inner = inner_ref[0]
    tail = jnp.exp(jnp.minimum(inner[-1:] - inner, 0.0)) * rates_ref[0]
    return spread(tail, width), spread(jnp.exp(inner), width)


def states_kernel(width, x_ref, dy_ref, inner_ref, rates_ref, b_ref, c_ref, out_ref):
    tail, growth = scales(inner_ref, rates_ref, width)
    for i, (keys_ref, rows) in enumerate(((b_ref, x_ref[...] * tail), (c_ref, dy_ref[...] * growth))):
        state = dot3(halves(keys_ref[...]), halves(rows), TN)
        for j in range(LANES // 128):
            out_ref[i, :, j] = state[:, j * 128 : (j + 1) * 128].reshape(-1, 8, 128)


def local_kernel(width, x_ref, dy_ref, inner_t_ref, rates_t_ref, inner_ref, rates_ref, skip_ref, b_ref, c_ref, y_ref, gx_ref, keys_ref, cb_ref, bc_ref, sum_ref):
    step = pl.program_id(0)
    tokens = x_ref.shape[0]
    per = LANES // width

    @pl.when(step == 0)
    def _():
        b, c = halves(b_ref[...]), halves(c_ref[...])
        cb_ref[...] = dot3(c, b, NT)
        bc_ref[...] = dot3(b, c, NT)
        sum_ref[...] = jnp.zeros_like(sum_ref)

    row = lax.broadcasted_iota(jnp.int32, (tokens, tokens), 0)
    col = lax.broadcasted_iota(jnp.int32, (tokens, tokens), 1)
    lane = lax.broadcasted_iota(jnp.int32, (tokens, 2 * width), 1)
    total = sum_ref[...]
    for pair in range(per // 2):
        at = slice(pair * 2 * width, (pair + 1) * 2 * width)
        x, dy = x_ref[:, at], dy_ref[:, at]
        y = skip_ref[:, at] * x
        gx = skip_ref[:, at] * dy
        x_parts, dy_parts = halves(x), halves(dy)
        for side in range(2):
            i = pair * 2 + side
            mine = (lane < width) if side == 0 else (lane >= width)
            zero = jnp.zeros((), jnp.bfloat16)
            x_own = tuple(jnp.where(mine, part, zero) for part in x_parts)
            dy_own = tuple(jnp.where(mine, part, zero) for part in dy_parts)
            down = jnp.broadcast_to(inner_t_ref[0, :, i : i + 1], (tokens, tokens))
            dt_down = jnp.broadcast_to(rates_t_ref[0, :, i : i + 1], (tokens, tokens))
            across = inner_ref[0, i : i + 1, :]
            gap = down - across
            within = jnp.where(row >= col, jnp.exp(jnp.minimum(gap, 0.0)), 0.0) * rates_ref[0, i : i + 1, :]
            turned = jnp.where(col >= row, jnp.exp(jnp.minimum(-gap, 0.0)), 0.0) * dt_down
            y = y + dot3(halves(within * cb_ref[...]), x_own)
            gx = gx + dot3(halves(turned * bc_ref[...]), dy_own)
            total = total + within * dot3(dy_own, x_parts, NT)
        y_ref[:, at] = y
        gx_ref[:, at] = gx
    sum_ref[...] = total

    @pl.when(step == pl.num_programs(0) - 1)
    def _():
        parts = halves(sum_ref[...])
        keys_ref[:tokens] = dot3(parts, halves(c_ref[...]), TN)
        keys_ref[tokens:] = dot3(parts, halves(b_ref[...]))


def finish_kernel(width, x_ref, dy_ref, inner_ref, rates_ref, b_ref, c_ref, low_ref, high_ref, y_ref, gx_ref, terms_ref, out_ref, grad_ref, keys_ref):
    step = pl.program_id(0)
    tokens = x_ref.shape[0]
    tail, growth = scales(inner_ref, rates_ref, width)

    def state(i):
        rows = [
            jnp.concatenate([ref[i, :, j].reshape(-1, 128) for j in range(LANES // 128)], axis=1)
            for ref in (low_ref, high_ref)
        ]
        return halves(jnp.concatenate(rows, axis=0))

    entering, adjoint = state(0), state(1)
    out_ref[...] = y_ref[...] + growth * dot3(halves(c_ref[...]), entering)
    grad_ref[...] = gx_ref[...] + tail * dot3(halves(b_ref[...]), adjoint)

    @pl.when(step == 0)
    def _():
        keys_ref[...] = terms_ref[...]

    keys_ref[:tokens] += dot3(halves(x_ref[...] * tail), adjoint, NT)
    keys_ref[tokens:] += dot3(halves(dy_ref[...] * growth), entering, NT)


def whole(shape):
    return pl.BlockSpec(shape, lambda i: (0,) * len(shape))


def exchange(states, log_decay, axis, meanwhile):
    size, mine = lax.axis_size(axis), lax.axis_index(axis)
    tiles = log_decay.shape[0]

    def send(values, logs, pairs):
        got = lax.ppermute(jnp.concatenate([values.reshape(-1, 128), logs], axis=0), axis, pairs)
        return got[:-tiles].reshape(values.shape), got[-tiles:]

    def decay(logs):
        return jnp.exp(logs)[None, :, None, :]

    kept, sides = [], []
    now, logs = states, log_decay
    for k in range(LEVELS):
        pairs = [(i, i ^ (1 << k)) for i in range(size)]
        right = ((mine >> k) & 1) == 1
        rows = now.shape[1] // 2
        low, high = now[:, :rows], now[:, rows:]
        own = jnp.where(right, high, low)
        got, other = send(jnp.where(right, low, high), logs, pairs)
        left_logs, right_logs = jnp.where(right, other, logs), jnp.where(right, logs, other)
        over_left, over_right = decay(left_logs), decay(right_logs)
        left_part, right_part = jnp.where(right, got, own), jnp.where(right, own, got)
        now = jnp.stack(
            [over_right * left_part[0] + right_part[0], left_part[1] + over_left * right_part[1]]
        )
        logs = left_logs + right_logs
        kept.append((left_part[0], right_part[1], over_left, over_right))
        sides.append((pairs, right))

    block = 1 << LEVELS
    count = size // block
    place = mine // block
    received, sources = [], []
    offsets = sorted(range(1, count), key=lambda d: -min(d, count - d))
    for d in offsets:
        pairs = [(i, (i + block * d) % size) for i in range(size)]
        received.append(send(jnp.where(place + d < count, now[0], now[1]), logs, pairs))
        sources.append((place - d) % count)
    aside = meanwhile()
    forward = jnp.zeros_like(now[0])
    backward = jnp.zeros_like(now[0])
    for d, (values, _), origin in zip(offsets, received, sources, strict=True):
        first, last = jnp.minimum(origin, place), jnp.maximum(origin, place)
        between = jnp.zeros_like(logs)
        for (_, other), source in zip(received, sources, strict=True):
            between = between + jnp.where((source > first) & (source < last), other, 0.0)
        term = decay(between) * values
        forward = forward + jnp.where(place >= d, term, 0.0)
        backward = backward + jnp.where(place >= d, 0.0, term)

    for k in reversed(range(LEVELS)):
        left_sum, right_sum, over_left, over_right = kept[k]
        pairs, right = sides[k]
        to_left = jnp.stack([forward, over_right * backward + right_sum])
        to_right = jnp.stack([over_left * forward + left_sum, backward])
        own = jnp.where(right, to_right, to_left)
        got = lax.ppermute(jnp.where(right, to_left, to_right), axis, pairs)
        low, high = jnp.where(right, got, own), jnp.where(right, own, got)
        if k:
            forward, backward = (jnp.concatenate([low[i], high[i]], axis=0) for i in range(2))
    return (low, high), aside


def body(inputs, rates, decay_rate, skip, keys_b, keys_c, grad_out):
    tokens, lanes = inputs.shape
    heads = rates.shape[0]
    width = lanes // heads
    state_size = keys_b.shape[1]
    grid = lanes // LANES
    per = LANES // width

    logs = -(decay_rate[:, None] * rates)
    upto = jnp.triu(jnp.ones((tokens, tokens), jnp.float32))
    inner = jnp.dot(logs, upto, precision=HIGHEST)
    total = jnp.sum(logs, axis=1)
    inner_rows, rates_rows = inner.reshape(grid, per, tokens), rates.reshape(grid, per, tokens)
    inner_t, rates_t = jnp.swapaxes(inner_rows, 1, 2), jnp.swapaxes(rates_rows, 1, 2)

    def on_lanes(of_heads):
        lane = jnp.arange(lanes).reshape(lanes // 128, 128, 1)
        return jnp.sum(jnp.where(lane // width == jnp.arange(heads), of_heads, 0.0), axis=2)

    tile = pl.BlockSpec((tokens, LANES), lambda i: (0, i))
    state_tile = pl.BlockSpec((2, state_size // 8, LANES // 128, 8, 128), lambda i: (0, 0, i, 0, 0))
    half_tile = pl.BlockSpec((2, state_size // 16, LANES // 128, 8, 128), lambda i: (0, 0, i, 0, 0))
    columns = pl.BlockSpec((1, tokens, per), lambda i: (i, 0, 0))
    keys = whole((tokens, state_size))
    big = jax.ShapeDtypeStruct((tokens, lanes), jnp.float32)
    params = pltpu.CompilerParams(dimension_semantics=("arbitrary",))

    states = pl.pallas_call(
        functools.partial(states_kernel, width),
        grid=(grid,),
        in_specs=[tile, tile, columns, columns, keys, keys],
        out_specs=state_tile,
        out_shape=jax.ShapeDtypeStruct((2, state_size // 8, lanes // 128, 8, 128), jnp.float32),
        compiler_params=params,
        cost_estimate=pl.CostEstimate(flops=12 * tokens * state_size * lanes, bytes_accessed=6 << 20, transcendentals=0),
        name="states",
    )(inputs, grad_out, inner_t, rates_t, keys_b, keys_c)

    small = pl.BlockSpec((1, per, tokens), lambda i: (i, 0, 0))
    local = pl.pallas_call(
        functools.partial(local_kernel, width),
        grid=(grid,),
        in_specs=[tile, tile, columns, columns, small, small, pl.BlockSpec((1, LANES), lambda i: (0, i)), keys, keys],
        out_specs=[tile, tile, whole((2 * tokens, state_size))],
        out_shape=[big, big, jax.ShapeDtypeStruct((2 * tokens, state_size), jnp.float32)],
        scratch_shapes=[pltpu.VMEM((tokens, tokens), jnp.float32)] * 3,
        compiler_params=params,
        cost_estimate=pl.CostEstimate(flops=18 * tokens * tokens * lanes, bytes_accessed=8 << 20, transcendentals=2 * tokens * tokens * heads),
        name="local",
    )
    skip_lanes = on_lanes(skip).reshape(1, lanes)

    def meanwhile():
        return local(inputs, grad_out, inner_t, rates_t, inner_rows, rates_rows, skip_lanes, keys_b, keys_c)

    (low, high), (y, gx, terms) = exchange(states, on_lanes(total), "seq", meanwhile)

    output, grad_x, key_terms = pl.pallas_call(
        functools.partial(finish_kernel, width),
        grid=(grid,),
        in_specs=[tile, tile, columns, columns, keys, keys, half_tile, half_tile, tile, tile, whole((2 * tokens, state_size))],
        out_specs=[tile, tile, whole((2 * tokens, state_size))],
        out_shape=[big, big, jax.ShapeDtypeStruct((2 * tokens, state_size), jnp.float32)],
        compiler_params=pltpu.CompilerParams(dimension_semantics=("arbitrary",), vmem_limit_bytes=20 << 20),
        cost_estimate=pl.CostEstimate(flops=24 * tokens * state_size * lanes, bytes_accessed=14 << 20, transcendentals=0),
        name="finish",
    )(inputs, grad_out, inner_t, rates_t, keys_b, keys_c, low, high, y, gx, terms)
    cores = lax.axis_size("head")
    summed = key_terms
    for d in range(1, cores):
        summed = summed + lax.ppermute(key_terms, "head", [(i, (i + d) % cores) for i in range(cores)])
    return output, grad_x, summed[:tokens], summed[tokens:]


def solution(mesh):
    in_specs = (
        P(("grp", "seq"), "head"),
        P("head", ("grp", "seq")),
        P("head"),
        P("head"),
        P(("grp", "seq"), None),
        P(("grp", "seq"), None),
        P(("grp", "seq"), "head"),
    )
    out_specs = (
        P(("grp", "seq"), "head"),
        P(("grp", "seq"), "head"),
        P(("grp", "seq"), None),
        P(("grp", "seq"), None),
    )
    return jax.shard_map(body, mesh=mesh, in_specs=in_specs, out_specs=out_specs, check_vma=False)
```
